768 devices in a mesh: aa: 6 (over z_hi, core), ba: 128 (over z_lo, y, x).
Axes of the slice: x: 4, y: 8, z: 12 (z_hi: 3, z_lo: 4; z = z_hi * 4 + z_lo), core: 2. Of those that a mesh axis runs over, the one named last changes fastest.
Arguments:
- queries: bfloat16 [6, 128, 192, 1024], P('aa', 'ba'), may hold values from -6 to 6
- key_rows: bfloat16 [6, 128, 192, 1024], P('aa', 'ba'), may hold values from -6 to 6
- value_rows: bfloat16 [6, 128, 192, 1024], P('aa', 'ba'), may hold values from -24 to 24
- out_proj: bfloat16 [6, 1024, 1024], P('aa', 'ba'), may hold values from -0.1875 to 0.1875
- scale_ids: int32 [128, 192], P('ba'), may hold values from 0 to 7, never falling along the last dimension, each value on 1 to 64 neighbouring positions
- residual_in: bfloat16 [128, 192, 1024], P('ba'), may hold values from -4 to 4
- cotangent: bfloat16 [128, 192, 1024], P('ba'), may hold values from -6 to 6
Outputs:
- residual_out: bfloat16 [6, 128, 192, 1024], P('aa', 'ba')
- grad_query: bfloat16 [6, 128, 192, 1024], P('aa', 'ba')
- grad_key: bfloat16 [6, 128, 192, 1024], P('aa', 'ba')
- grad_value: bfloat16 [6, 128, 192, 1024], P('aa', 'ba')
- grad_proj: float32 [6, 1024, 1024], P('aa', 'ba')
The draws below stay inside these ranges and needn't reach their ends.
Inputs may be any that keep to these rules, and one draw needn't show every extreme that they name: `scale_ids`: for each image the scale ids never fall along the tokens; every scale from 0 to 7 is present, with 1 to 64 tokens.
All inputs are finite; a program needn't handle non-finite values.
Results may differ from the reference program's by a relative error of at most 0.0086.
Values may be sent and summed in bfloat16 or wider, within the bound.
A program may use at most 64 MiB of HBM per device.

```python
import math
import jax
import jax.numpy as jnp
import numpy as np
from jax import lax

HEADS = 16
HD = 64
RES = 1024
SEQ = 192
SCALES = 8
MOST = 64
INNER = 1024
IMAGES = 128
SECTIONS = 6


def query_key_pair(key):
    seeded = jax.random.fold_in(key, 9173)
    full_shape = (SECTIONS, IMAGES, SEQ, HEADS * HD)
    queries = jnp.clip(jax.random.normal(jax.random.fold_in(seeded, 5), full_shape, jnp.float32), -5.0, 5.0)
    key_rows = jnp.clip(jax.random.normal(jax.random.fold_in(seeded, 6), full_shape, jnp.float32), -5.0, 5.0)
    return (queries, key_rows)


def draw_queries(key, part):
    return query_key_pair(key)[0].astype(jnp.bfloat16)


def draw_key_rows(key, part):
    return query_key_pair(key)[1].astype(jnp.bfloat16)


def spiked(entries, key, source, target, parts, factor):
    def block_of(dim):
        return (jnp.arange(entries.shape[dim]) // (entries.shape[dim] // parts)).reshape((-1,) + (1,) * (entries.ndim - 1 - dim))

    near = jax.random.permutation(key, parts)[block_of(target)]
    far = (block_of(target) + parts // 2) % parts
    return jnp.where((block_of(source) == near) | (block_of(source) == far), factor * entries, entries)


def steps_of(rng, dims, split, smallest, high):
    loudness = 1.0
    for position, parts in split:
        draws = jax.random.uniform(jax.random.fold_in(jax.random.fold_in(rng, 6), position), (parts,), jnp.float32, smallest / len(split), high / len(split))
        loudness = loudness * jnp.repeat(jnp.exp(draws), dims[position] // parts).reshape((-1,) + (1,) * (len(dims) - 1 - position))
    return loudness


def length_profile(amount, total, most, lean):
    weights = [(1 << 20) // math.isqrt(rank ** lean) + 1 for rank in range(2, amount + 1)]
    rest, holding = total - most - (amount - 1), [1] * (amount - 1)
    while rest > 0:
        free = [i for i in range(amount - 1) if holding[i] < most]
        whole, budget = sum([weights[i] for i in free]), rest
        for i in free:
            more = min(most - holding[i], max(1, budget * weights[i] // whole), rest)
            holding[i] = holding[i] + more
            rest = rest - more
    return np.array([most] + holding)


def uneven(stream_key, count, total, reach, lean):
    if count == 2:
        one = jax.random.randint(stream_key, (), max(1, total - reach), min(reach, total - 1) + 1)
        return jnp.stack([one, total - one])
    tallies = jnp.asarray(length_profile(count, total, reach, lean), jnp.int32)
    couples = (count - 1) // 2
    donor, receiver = tallies[1:1 + 2 * couples:2], tallies[2:2 + 2 * couples:2]
    margin = jnp.minimum(donor - 1, reach - receiver)
    moved = jax.random.randint(jax.random.fold_in(stream_key, 1), (couples,), 0, 1 << 20) % (margin + 1)
    tallies = tallies.at[1:1 + 2 * couples:2].set(donor - moved).at[2:2 + 2 * couples:2].set(receiver + moved)
    return tallies[jax.random.permutation(jax.random.fold_in(stream_key, 2), count)]


def gaussian(key, extent, scale, limit, pieces=(), held_as=jnp.bfloat16):
    entries = jax.random.normal(key, extent, jnp.float32) * scale
    if len(pieces) > 0:
        entries = steps_of(key, extent, pieces, -0.22, 0.18) * entries
    return jnp.clip(entries, min=-limit, max=limit).astype(held_as)


def bell_draw_with(key, shape, scale, reach, pieces, heavy, held_as=jnp.bfloat16):
    array = scale * jax.random.normal(key, shape, jnp.float32)
    if pieces:
        array = array * steps_of(key, shape, pieces, -0.22, 0.18)
    return jnp.clip(spiked(array, jax.random.fold_in(key, 3), *heavy), -reach, reach).astype(held_as)


def setup_inputs(seed: int = 0) -> dict:
    keys = jax.random.split(jax.random.key(seed), 8)
    queries = draw_queries(jax.random.fold_in(keys[7], 71), 0)
    key_rows = draw_key_rows(jax.random.fold_in(keys[7], 71), 0)
    value_rows = bell_draw_with(keys[2], (SECTIONS, IMAGES, SEQ, INNER), 1.0, 24.0, ((0, 6), (1, 128)), (1, 3, 128, 5.5))
    out_proj = gaussian(keys[3], (SECTIONS, INNER, RES), INNER ** -0.5, 0.1875, ((0, 6), (1, 128)))
    scale_ids = jax.vmap(lambda own: jnp.searchsorted(jnp.cumsum(uneven(own, SCALES, SEQ, MOST, 2)), jnp.arange(SEQ), side="right"))(jax.random.split(keys[4], IMAGES)).reshape((IMAGES, SEQ)).astype(jnp.int32)
    residual_in = gaussian(keys[5], (IMAGES, SEQ, RES), 0.3, 4.0, ((0, 128),))
    cotangent = gaussian(keys[6], (IMAGES, SEQ, RES), 1.0, 6.0, ((0, 128),))
    return dict(queries=queries, key_rows=key_rows, value_rows=value_rows, out_proj=out_proj, scale_ids=scale_ids, residual_in=residual_in, cotangent=cotangent)


def round_low(values):
    return lax.optimization_barrier(values.astype(jnp.bfloat16)).astype(jnp.float32)


def reference(queries, key_rows, value_rows, out_proj, scale_ids, residual_in, cotangent):
    images = scale_ids.shape[0]
    length = scale_ids.shape[1]
    score_scale = HD ** -0.5
    visible = scale_ids[:, None, :] <= scale_ids[:, :, None]
    cot_rows = cotangent.reshape(images * length, RES)

    def section_pass(running, operands):
        q_all, k_all, v_all, w_out = operands
        q_heads = q_all.reshape(images, length, HEADS, HD).astype(jnp.float32)
        k_heads = k_all.reshape(images, length, HEADS, HD).astype(jnp.float32)
        v_heads = v_all.reshape(images, length, HEADS, HD).astype(jnp.float32)
        scores = jnp.einsum("bihd,bjhd->bhij", q_heads, k_heads) * score_scale
        scores = jnp.where(visible[:, None], scores, -jnp.inf)
        row_max = jnp.max(scores, axis=-1, keepdims=True)
        lifted = jnp.exp(scores - row_max)
        attn_probs = lifted / jnp.sum(lifted, axis=-1, keepdims=True)
        probs_low = round_low(attn_probs)
        attended = jnp.einsum("bhij,bjhd->bihd", probs_low, v_heads)
        attended = attended.astype(jnp.bfloat16).reshape(images * length, INNER)
        branch = jnp.dot(attended, w_out, preferred_element_type=jnp.float32)
        running_next = running + branch.reshape(images, length, RES)
        d_attn = round_low(jnp.dot(cot_rows, w_out.T, preferred_element_type=jnp.float32))
        grad_proj = lax.dot_general(attended, cot_rows, (((0,), (0,)), ((), ())), preferred_element_type=jnp.float32) / IMAGES
        d_heads = d_attn.reshape(images, length, HEADS, HD)
        grad_value = jnp.einsum("bhij,bihd->bjhd", probs_low, d_heads)
        d_probs = jnp.einsum("bihd,bjhd->bhij", d_heads, v_heads)
        row_delta = jnp.sum(attn_probs * d_probs, axis=-1, keepdims=True)
        d_scores = round_low(attn_probs * (d_probs - row_delta) * score_scale)
        grad_query = jnp.einsum("bhij,bjhd->bihd", d_scores, k_heads)
        grad_key = jnp.einsum("bhij,bihd->bjhd", d_scores, q_heads)
        outputs = (
            running_next.astype(jnp.bfloat16),
            grad_query.reshape(images, length, INNER).astype(jnp.bfloat16),
            grad_key.reshape(images, length, INNER).astype(jnp.bfloat16),
            grad_value.reshape(images, length, INNER).astype(jnp.bfloat16),
            grad_proj,
        )
        return running_next, outputs

    start_value = residual_in.astype(jnp.float32)
    final_value, stacked = lax.scan(section_pass, start_value, (queries, key_rows, value_rows, out_proj))
    return stacked[0], stacked[1], stacked[2], stacked[3], stacked[4]
```

```python
import jax
import jax.numpy as jnp
from jax import lax
from jax.experimental import pallas as pl
from jax.experimental.pallas import tpu as pltpu
from jax.sharding import Mesh
from jax.sharding import PartitionSpec as P

AXES = ("zh", "core", "zl", "y", "x")
AA = ("zh", "core")
BA = ("zl", "y", "x")
SIZE = {"zh": 3, "core": 2, "zl": 4, "y": 8, "x": 4}
MESH = pl.DeviceIdType.MESH
BF = jnp.bfloat16
F32 = jnp.float32
T = 192
D = 1024
PAIRS = 8
HALF = 512
ROWS = 96
COPIES = 128


def mm(a, b, ca, cb):
    return lax.dot_general(a, b, (((ca,), (cb,)), ((), ())), preferred_element_type=F32)


def moved(axis, by):
    n = SIZE[axis]
    return lax.rem(lax.axis_index(axis) + (by % n), n)


class Net:
    def __init__(self, send, recv):
        self.send, self.recv, self.used, self.sent = send, recv, 0, []

    def copy(self, src, dst, axis, by, when=None):
        i = self.used
        self.used += 1
        c = pltpu.make_async_remote_copy(
            src_ref=src,
            dst_ref=dst,
            send_sem=self.send.at[i],
            recv_sem=self.recv.at[i],
            device_id={axis: moved(axis, by)},
            device_id_type=MESH,
        )
        if when is None:
            c.start()
        else:
            pl.when(when)(c.start)
        self.sent.append((c, when))
        return c

    def drain(self):
        for c, when in self.sent:
            if when is None:
                c.wait_send()
            else:
                pl.when(when)(c.wait_send)


def kernel(
    q_hbm, k_hbm, v_hbm, w_hbm, ids_ref, res_hbm, cot_hbm,
    ro_hbm, gq_hbm, gk_hbm, gv_hbm, gp_ref,
    q, k, v, res, cot, wbuf, bias, probs, att, datt, gq, gk, gv, ro,
    prod, y1p, y1m, y1, x1r, x1, z1r, x2r, y2p, y2m, y2s, y2, z2r,
    br, bl, bo, ph, pr,
    in_sem, out_sem, send_sem, recv_sem,
):
    zh, core = lax.axis_index("zh"), lax.axis_index("core")
    z, y, x = (lax.axis_index(a) for a in BA)
    net = Net(send_sem, recv_sem)

    def yy(by):
        return moved("y", by)

    own_w = pltpu.make_async_copy(w_hbm, wbuf.at[z, y, x], in_sem.at[0])
    own_w.start()
    loads = []
    for i, (src, dst) in enumerate(((q_hbm, q), (k_hbm, k), (v_hbm, v), (cot_hbm, cot), (res_hbm, res))):
        c = pltpu.make_async_copy(src, dst, in_sem.at[i + 1])
        c.start()
        loads.append(c)

    barrier = pltpu.get_barrier_semaphore()
    greeted = [("zl", d) for d in (1, 2, 3)] + [("x", d) for d in (1, 2, 3)]
    greeted += [("y", 1), ("y", -1), ("zh", 1), ("zh", 2), ("core", 1)]
    for axis, by in greeted:
        pl.semaphore_signal(barrier, 1, device_id={axis: moved(axis, by)}, device_id_type=MESH)

    ids = jnp.broadcast_to(ids_ref[...], (T, T))
    row = lax.broadcasted_iota(jnp.int32, (T, T), 0)
    lane = lax.broadcasted_iota(jnp.int32, (T, T), 1)
    ids_t = jnp.sum(jnp.where(row == lane, ids, 0).astype(F32), axis=1, keepdims=True)
    bias[...] = jnp.where(jnp.broadcast_to(ids_t, (T, T)) <= ids.astype(F32), 0.0, -1e30)
    first = lax.broadcasted_iota(jnp.int32, (T, 128), 1) < 64

    own_w.wait()
    pl.semaphore_wait(barrier, len(greeted))

    lo, hi = pl.ds(0, HALF), pl.ds(HALF, HALF)

    own = wbuf.at[z, y, x]
    zc = [net.copy(own, own, "zl", d) for d in (1, 2, 3)]

    def halves(val):
        zero = jnp.zeros_like(val)
        return (jnp.where(first, val, zero), jnp.where(first, zero, val))

    def forward(lo_pair, hi_pair):
        def body(h, _):
            sl = pl.ds(pl.multiple_of(h * 128, 128), 128)
            qp = q[:, sl]
            out = jnp.zeros((T, 128), F32)
            for a, (kh, vh) in enumerate(zip(halves(k[:, sl]), halves(v[:, sl]))):
                s = mm(kh, qp, 1, 1) * 0.125 + bias[...]
                e = jnp.exp(s - jnp.max(s, axis=0, keepdims=True))
                p = (e * (1.0 / jnp.sum(e, axis=0, keepdims=True))).astype(BF)
                probs[2 * h + a] = p
                out = out + mm(p, vh, 0, 0)
            att[:, sl] = out.astype(BF)
            return 0

        lax.fori_loop(lo_pair, hi_pair, body, 0)

    def backward(lo_pair, hi_pair):
        def body(h, _):
            sl = pl.ds(pl.multiple_of(h * 128, 128), 128)
            dop = datt[:, sl]
            dv = jnp.zeros((T, 128), F32)
            dk = jnp.zeros((T, 128), F32)
            dq = jnp.zeros((T, 128), F32)
            parts = zip(halves(q[:, sl]), halves(k[:, sl]), halves(v[:, sl]), halves(dop))
            for a, (qh, kh, vh, dh) in enumerate(parts):
                pb = probs[2 * h + a]
                dp = mm(vh, dop, 1, 1)
                p = pb.astype(F32)
                delta = jnp.sum(p * dp, axis=0, keepdims=True)
                ds = (p * (dp - delta) * 0.125).astype(BF)
                dv = dv + mm(pb, dh, 1, 0)
                dk = dk + mm(ds, qh, 1, 0)
                dq = dq + mm(ds, kh, 0, 0)
            gq[:, sl] = dq.astype(BF)
            gk[:, sl] = dk.astype(BF)
            gv[:, sl] = dv.astype(BF)
            return 0

        lax.fori_loop(lo_pair, hi_pair, body, 0)

    for c in loads:
        c.wait()
    forward(0, 2)
    for c in zc:
        c.wait_recv()

    def block(cols, by):
        return wbuf.at[:, yy(by), x, :, cols]

    x1c = [net.copy(block(lo, 0), block(lo, 0), "x", d) for d in (1, 2, 3)]
    x2c = []

    def spread(by):
        for d in (1, 2, 3):
            x2c.append(net.copy(block(hi, by), block(hi, by), "x", d))

    def hop2(t):
        up = net.copy(block(hi, 1 - t), block(hi, 1 - t), "y", 1) if t <= 3 else None
        down = net.copy(block(hi, t - 1), block(hi, t - 1), "y", -1)
        return up, down

    def hop1(t):
        cs = []
        for s in range(2):
            cols = pl.ds(256 * s, 256)
            b = wbuf.at[:, yy(1 - t), :, :, cols]
            cs.append(net.copy(b, b, "y", 1))
            if t <= 3:
                b = wbuf.at[:, yy(t - 1), :, :, cols]
                cs.append(net.copy(b, b, "y", -1))
        return cs

    c2 = hop2(1)
    spread(0)
    forward(2, 4)
    for c in x1c:
        c.wait_recv()
    c1 = hop1(1)
    forward(4, 5)
    for t in range(1, 5):
        up, down = c2
        down.wait_recv()
        if up is not None:
            up.wait_recv()
        if t <= 3:
            c2 = hop2(t + 1)
        if up is not None:
            spread(-t)
        spread(t)
        if t <= 3:
            for c in c1:
                c.wait_recv()
            c1 = hop1(t + 1)
        if t <= 3:
            forward(4 + t, 5 + t)

    for i in range(4):
        pz = mm(att[:, pl.ds(256 * i, 256)], cot[...], 0, 0)
        prod[i] = pz.reshape(8, 4, 8, D).astype(BF)

    def red1(sign, steps, bufs):
        def step(t, got):
            d = yy(sign * (steps + 1 - t))
            cs = []
            for s in range(2):
                cols = pl.ds(256 * s, 256)
                if t == 1:
                    src = prod.at[:, d, :, :, cols]
                else:
                    got[s].wait_recv()
                    src = bufs.at[t - 2, :, :, :, cols]
                    total = src[...].astype(F32) + prod[:, d, :, :, cols].astype(F32)
                    bufs[t - 2, :, :, :, cols] = total.astype(BF)
                cs.append(net.copy(src, bufs.at[t - 1, :, :, :, cols], "y", sign))
            return cs

        return step

    up1, down1 = red1(1, 4, y1p), red1(-1, 3, y1m)
    u1, d1 = up1(1, None), down1(1, None)

    x2sent = {}
    for by in (-4, 3, -3, 2, -2, 1, -1, 0):
        d = yy(by)
        x2sent[by] = [
            net.copy(prod.at[:, d, moved("x", dx), :, hi], x2r.at[dx - 1, :, d], "x", dx) for dx in (1, 2, 3)
        ]

    def x2sum(by):
        for c in x2sent[by]:
            c.wait_recv()
        d = yy(by)
        total = prod[:, d, x, :, hi].astype(F32)
        for j in range(3):
            total = total + x2r[j, :, d].astype(F32)
        return total

    for c in c1 + x2c:
        c.wait_recv()

    w_all = wbuf[...].reshape(D, D)
    a_all = att[...]
    other = pl.ds(0, T)
    swaps = []
    for h in range(2):
        cols = pl.ds(HALF * h, HALF)
        b = mm(a_all, w_all[:, HALF * h : HALF * h + HALF], 1, 0)
        br[:, cols] = b
        bl[:, cols] = b.astype(BF)
        swaps.append(net.copy(bl.at[:, cols], bo.at[:, cols], "core", 1))
    datt[...] = mm(cot[...], w_all, 1, 1).astype(BF)
    mine = pl.ds(pl.multiple_of(core * ROWS, 8), ROWS)
    far = []
    for h in range(2):
        cols = pl.ds(HALF * h, HALF)
        swaps[h].wait_recv()
        ph[:, cols] = (br[mine, cols] + bo[mine, cols].astype(F32)).astype(BF)
        near = net.copy(ph.at[:, cols], pr.at[0, mine, cols], "zh", 1, when=zh < 2)
        skip = net.copy(ph.at[:, cols], pr.at[1, mine, cols], "zh", 2, when=zh == 0)
        far.append((near, skip))

    def up2(t, got):
        d = 4 - t
        total = x2sum(d)
        if t > 1:
            got.wait_recv()
            total = total + y2p[t - 2].astype(F32)
        y2s[t - 1] = total.astype(BF)
        return net.copy(y2s.at[t - 1], y2p.at[t - 1], "y", 1)

    def down2(t, got):
        d = t - 5
        total = x2sum(d)
        if t > 1:
            got.wait_recv()
            total = total + y2m[t - 2].astype(F32)
        y2s[2 + t] = total.astype(BF)
        return net.copy(y2s.at[2 + t], y2m.at[t - 1], "y", -1)

    u2 = d2 = None
    for t in range(1, 5):
        d2 = down2(t, d2)
        if t <= 3:
            u2 = up2(t, u2)
        if t <= 3:
            u1 = up1(t + 1, u1)
        if t <= 2:
            d1 = down1(t + 1, d1)
        backward(2 * t - 2, 2 * t)
    outs = []

    def store(i, src, dst):
        c = pltpu.make_async_copy(src, dst, out_sem.at[i])
        c.start()
        outs.append(c)

    store(0, gq, gq_hbm)
    store(1, gk, gk_hbm)
    store(2, gv, gv_hbm)

    for c in u1 + d1:
        c.wait_recv()
    y1[...] = (prod[:, y, :, :, lo].astype(F32) + y1p[3].astype(F32) + y1m[2].astype(F32)).astype(BF)
    x1c = [net.copy(y1.at[:, moved("x", dx)], x1r.at[dx - 1], "x", dx) for dx in (1, 2, 3)]

    total = x2sum(0)
    u2.wait_recv()
    d2.wait_recv()
    total = total + y2p[2].astype(F32) + y2m[3].astype(F32)
    y2[...] = total.astype(BF)
    z2c = [net.copy(y2.at[moved("zl", dz)], z2r.at[dz - 1], "zl", dz) for dz in (1, 2, 3)]

    for c in x1c:
        c.wait_recv()
    total = y1[:, x].astype(F32)
    for j in range(3):
        total = total + x1r[j].astype(F32)
    x1[...] = total.astype(BF)
    z1c = [net.copy(x1.at[moved("zl", dz)], z1r.at[dz - 1], "zl", dz) for dz in (1, 2, 3)]

    for cols, last, sums, got in ((hi, y2, z2r, z2c), (lo, x1, z1r, z1c)):
        for c in got:
            c.wait_recv()
        total = last[z].astype(F32)
        for j in range(3):
            total = total + sums[j].astype(F32)
        gp_ref[:, cols] = total * (1.0 / 128.0)

    passed = []
    for h in range(2):
        cols = pl.ds(HALF * h, HALF)
        near, skip = far[h]
        pl.when(zh > 0)(near.wait_recv)
        a = pr.at[0, mine, cols]
        passed.append((net.copy(a, a, "core", 1, when=zh > 0), zh > 0))
        pl.when(zh == 2)(skip.wait_recv)
        a = pr.at[1, mine, cols]
        passed.append((net.copy(a, a, "core", 1, when=zh == 2), zh == 2))
    br[...] = br[...] + res[...].astype(F32)

    @pl.when(core == 1)
    def _():
        br[...] = br[...] + bo[...].astype(F32)

    for c, when in passed:
        pl.when(when)(c.wait_recv)

    @pl.when(zh > 0)
    def _():
        br[...] = br[...] + pr[0].astype(F32)

    @pl.when(zh == 2)
    def _():
        br[...] = br[...] + pr[1].astype(F32)

    ro[...] = br[...].astype(BF)
    store(3, ro, ro_hbm)
    net.drain()
    for c in outs:
        c.wait()


def local(queries, key_rows, value_rows, out_proj, scale_ids, residual_in, cotangent):
    anyspace = pl.BlockSpec(memory_space=pl.ANY)
    vmem = pl.BlockSpec(memory_space=pltpu.VMEM)
    act = jax.ShapeDtypeStruct((T, D), BF)
    V = pltpu.VMEM
    scratch = [V((T, D), BF)] * 5 + [
        V((4, 8, 4, 8, D), BF),
        V((T, T), F32),
        V((16, T, T), BF),
    ] + [V((T, D), BF)] * 6 + [
        V((4, 8, 4, 8, D), BF),
        V((4, 4, 4, 8, HALF), BF),
        V((3, 4, 4, 8, HALF), BF),
        V((4, 4, 8, HALF), BF),
        V((3, 4, 8, HALF), BF),
        V((4, 8, HALF), BF),
        V((3, 8, HALF), BF),
        V((3, 4, 8, 8, HALF), BF),
        V((3, 4, 8, HALF), BF),
        V((4, 4, 8, HALF), BF),
        V((7, 4, 8, HALF), BF),
        V((4, 8, HALF), BF),
        V((3, 8, HALF), BF),
        V((T, D), F32),
        V((T, D), BF),
        V((T, D), BF),
        V((ROWS, D), BF),
        V((2, T, D), BF),
        pltpu.SemaphoreType.DMA((6,)),
        pltpu.SemaphoreType.DMA((4,)),
        pltpu.SemaphoreType.DMA((COPIES,)),
        pltpu.SemaphoreType.DMA((COPIES,)),
    ]
    ro, gq, gk, gv, gp = pl.pallas_call(
        kernel,
        out_shape=(act, act, act, act, jax.ShapeDtypeStruct((8, D), F32)),
        in_specs=[anyspace] * 4 + [vmem] + [anyspace] * 2,
        out_specs=(anyspace, anyspace, anyspace, anyspace, vmem),
        scratch_shapes=scratch,
        compiler_params=pltpu.CompilerParams(
            collective_id=0, has_side_effects=True, vmem_limit_bytes=56 << 20
        ),
        name="fused",
    )(
        queries.reshape(T, D), key_rows.reshape(T, D), value_rows.reshape(T, D), out_proj.reshape(8, D),
        scale_ids, residual_in.reshape(T, D), cotangent.reshape(T, D),
    )
    lead = (1, 1, T, D)
    return ro.reshape(lead), gq.reshape(lead), gk.reshape(lead), gv.reshape(lead), gp.reshape(1, 8, D)


def solution(mesh):
    torus = Mesh(mesh.devices.reshape(tuple(SIZE[a] for a in AXES)), AXES)
    act = P(AA, BA, None, None)
    return jax.shard_map(
        local,
        mesh=torus,
        in_specs=(act, act, act, P(AA, BA, None), P(BA, None), P(BA, None, None), P(BA, None, None)),
        out_specs=(act, act, act, act, P(AA, BA, None)),
        check_vma=False,
    )
```

```python
import jax
import jax.numpy as jnp
from jax import lax
from jax.experimental import pallas as pl
from jax.experimental.pallas import tpu as pltpu
from jax.sharding import Mesh
from jax.sharding import PartitionSpec as P

AXES = ("zh", "core", "zl", "y", "x")
AA = ("zh", "core")
BA = ("zl", "y", "x")
SIZE = {"zh": 3, "core": 2, "zl": 4, "y": 8, "x": 4}
MESH = pl.DeviceIdType.MESH
BF = jnp.bfloat16
F32 = jnp.float32
T = 192
D = 1024
PAIRS = 8
HALF = 512
ROWS = 96
COPIES = 144


def mm(a, b, ca, cb):
    return lax.dot_general(a, b, (((ca,), (cb,)), ((), ())), preferred_element_type=F32)


def moved(axis, by):
    n = SIZE[axis]
    return lax.rem(lax.axis_index(axis) + (by % n), n)


class Net:
    def __init__(self, send, recv):
        self.send, self.recv, self.used, self.sent = send, recv, 0, []

    def copy(self, src, dst, axis, by, when=None):
        i = self.used
        self.used += 1
        c = pltpu.make_async_remote_copy(
            src_ref=src,
            dst_ref=dst,
            send_sem=self.send.at[i],
            recv_sem=self.recv.at[i],
            device_id={axis: moved(axis, by)},
            device_id_type=MESH,
        )
        if when is None:
            c.start()
        else:
            pl.when(when)(c.start)
        self.sent.append((c, when))
        return c

    def drain(self):
        for c, when in self.sent:
            if when is None:
                c.wait_send()
            else:
                pl.when(when)(c.wait_send)


def kernel(
    q_hbm, k_hbm, v_hbm, w_hbm, ids_ref, res_hbm, cot_hbm,
    ro, gq, gk, gv, gp_ref,
    q, k, v, res, cot, wbuf, bias, probs, att, datt,
    prod, y1p, y1m, y1, x1r, x1, z1r, x2r, y2p, y2m, y2s, y2, z2r,
    br, bl, bo, ph, pr,
    in_sem, send_sem, recv_sem, ready,
):
    zh, core = lax.axis_index("zh"), lax.axis_index("core")
    z, y, x = (lax.axis_index(a) for a in BA)
    net = Net(send_sem, recv_sem)

    def yy(by):
        return moved("y", by)

    own_w = pltpu.make_async_copy(w_hbm, wbuf.at[z, y, x], in_sem.at[0])
    own_w.start()
    loads = []
    for i, (src, dst) in enumerate(((q_hbm, q), (k_hbm, k), (v_hbm, v), (cot_hbm, cot), (res_hbm, res))):
        c = pltpu.make_async_copy(src, dst, in_sem.at[i + 1])
        c.start()
        loads.append(c)

    barrier = pltpu.get_barrier_semaphore()
    greeted = [("zl", d) for d in (1, 2, 3)] + [("x", d) for d in (1, 2, 3)]
    greeted += [("y", 1), ("y", -1), ("core", 1)]

    def signal(sem, axis, by):
        pl.semaphore_signal(sem, 1, device_id={axis: moved(axis, by)}, device_id_type=MESH)

    for axis, by in greeted:
        signal(barrier, axis, by)
    pl.when(zh < 2)(lambda: signal(barrier, "zh", 1))
    pl.when(zh == 0)(lambda: signal(barrier, "zh", 2))

    ids = jnp.broadcast_to(ids_ref[...], (T, T))
    row = lax.broadcasted_iota(jnp.int32, (T, T), 0)
    lane = lax.broadcasted_iota(jnp.int32, (T, T), 1)
    ids_t = jnp.sum(jnp.where(row == lane, ids, 0).astype(F32), axis=1, keepdims=True)
    bias[...] = jnp.where(jnp.broadcast_to(ids_t, (T, T)) <= ids.astype(F32), 0.0, -1e30)
    first = lax.broadcasted_iota(jnp.int32, (T, 128), 1) < 64

    own_w.wait()
    pl.semaphore_wait(barrier, len(greeted) + zh)
    pl.when(zh > 0)(lambda: signal(ready.at[0], "zh", -1))
    pl.when(zh == 2)(lambda: signal(ready.at[1], "zh", -2))

    lo, hi = pl.ds(0, HALF), pl.ds(HALF, HALF)

    own = wbuf.at[z, y, x]
    zc = [net.copy(own, own, "zl", d) for d in (1, 2, 3)]

    def halves(val):
        zero = jnp.zeros_like(val)
        return (jnp.where(first, val, zero), jnp.where(first, zero, val))

    def forward(lo_pair, hi_pair):
        def body(h, _):
            sl = pl.ds(pl.multiple_of(h * 128, 128), 128)
            qp = q[:, sl]
            out = jnp.zeros((T, 128), F32)
            for a, (kh, vh) in enumerate(zip(halves(k[:, sl]), halves(v[:, sl]))):
                s = mm(kh, qp, 1, 1) * 0.125 + bias[...]
                e = jnp.exp(s - jnp.max(s, axis=0, keepdims=True))
                p = (e * (1.0 / jnp.sum(e, axis=0, keepdims=True))).astype(BF)
                probs[2 * h + a] = p
                out = out + mm(p, vh, 0, 0)
            att[:, sl] = out.astype(BF)
            return 0

        lax.fori_loop(lo_pair, hi_pair, body, 0)

    def backward(lo_pair, hi_pair):
        def body(h, _):
            sl = pl.ds(pl.multiple_of(h * 128, 128), 128)
            dop = datt[:, sl]
            dv = jnp.zeros((T, 128), F32)
            dk = jnp.zeros((T, 128), F32)
            dq = jnp.zeros((T, 128), F32)
            parts = zip(halves(q[:, sl]), halves(k[:, sl]), halves(v[:, sl]), halves(dop))
            for a, (qh, kh, vh, dh) in enumerate(parts):
                pb = probs[2 * h + a]
                dp = mm(vh, dop, 1, 1)
                p = pb.astype(F32)
                delta = jnp.sum(p * dp, axis=0, keepdims=True)
                ds = (p * (dp - delta) * 0.125).astype(BF)
                dv = dv + mm(pb, dh, 1, 0)
                dk = dk + mm(ds, qh, 1, 0)
                dq = dq + mm(ds, kh, 0, 0)
            gq[:, sl] = dq.astype(BF)
            gk[:, sl] = dk.astype(BF)
            gv[:, sl] = dv.astype(BF)
            return 0

        lax.fori_loop(lo_pair, hi_pair, body, 0)

    for c in loads:
        c.wait()
    forward(0, 2)
    for c in zc:
        c.wait_recv()

    def block(cols, by):
        return wbuf.at[:, yy(by), x, :, cols]

    x1c = [net.copy(block(lo, 0), block(lo, 0), "x", d) for d in (1, 2, 3)]
    x2c = []

    def spread(by):
        for d in (1, 2, 3):
            x2c.append(net.copy(block(hi, by), block(hi, by), "x", d))

    def hop2(t):
        up = net.copy(block(hi, 1 - t), block(hi, 1 - t), "y", 1) if t <= 3 else None
        down = net.copy(block(hi, t - 1), block(hi, t - 1), "y", -1)
        return up, down

    def hop1(t, got):
        cs = {}
        for s in range(4):
            cols = pl.ds(128 * s, 128)
            for sign in (1, -1):
                if t == 4 and (s < 2) != (sign == 1):
                    continue
                if got is not None:
                    got[sign, s].wait_recv()
                b = wbuf.at[:, yy(sign * (1 - t)), :, :, cols]
                cs[sign, s] = net.copy(b, b, "y", sign)
        if got is not None:
            for key in got:
                if key not in cs:
                    got[key].wait_recv()
        return cs

    c2 = hop2(1)
    spread(0)
    forward(2, 4)
    for c in x1c:
        c.wait_recv()
    c1 = hop1(1, None)
    forward(4, 5)
    for t in range(1, 5):
        up, down = c2
        down.wait_recv()
        if up is not None:
            up.wait_recv()
        if t <= 3:
            c2 = hop2(t + 1)
        if up is not None:
            spread(-t)
        spread(t)
        if t <= 3:
            c1 = hop1(t + 1, c1)
        if t <= 3:
            forward(4 + t, 5 + t)

    for i in range(4):
        pz = mm(att[:, pl.ds(256 * i, 256)], cot[...], 0, 0)
        prod[i] = pz.reshape(8, 4, 8, D).astype(BF)

    def red1(sign, steps, bufs):
        def step(t, got):
            d = yy(sign * (steps + 1 - t))
            cs = []
            for s in range(2):
                cols = pl.ds(256 * s, 256)
                if t == 1:
                    src = prod.at[:, d, :, :, cols]
                else:
                    got[s].wait_recv()
                    src = bufs.at[t - 2, :, :, :, cols]
                    total = src[...].astype(F32) + prod[:, d, :, :, cols].astype(F32)
                    bufs[t - 2, :, :, :, cols] = total.astype(BF)
                cs.append(net.copy(src, bufs.at[t - 1, :, :, :, cols], "y", sign))
            return cs

        return step

    up1, down1 = red1(1, 4, y1p), red1(-1, 3, y1m)
    u1, d1 = up1(1, None), down1(1, None)

    x2sent = {}
    for by in (-4, 3, -3, 2, -2, 1, -1, 0):
        d = yy(by)
        x2sent[by] = [
            net.copy(prod.at[:, d, moved("x", dx), :, hi], x2r.at[dx - 1, :, d], "x", dx) for dx in (1, 2, 3)
        ]

    def x2sum(by):
        for c in x2sent[by]:
            c.wait_recv()
        d = yy(by)
        total = prod[:, d, x, :, hi].astype(F32)
        for j in range(3):
            total = total + x2r[j, :, d].astype(F32)
        return total

    for c in list(c1.values()) + x2c:
        c.wait_recv()

    w_all = wbuf[...].reshape(D, D)
    a_all = att[...]
    other = pl.ds(0, T)
    swaps = []
    for h in range(2):
        cols = pl.ds(HALF * h, HALF)
        b = mm(a_all, w_all[:, HALF * h : HALF * h + HALF], 1, 0)
        br[:, cols] = b
        bl[:, cols] = b.astype(BF)
        swaps.append(net.copy(bl.at[:, cols], bo.at[:, cols], "core", 1))
    datt[...] = mm(cot[...], w_all, 1, 1).astype(BF)
    mine = pl.ds(pl.multiple_of(core * ROWS, 8), ROWS)
    far = []
    pl.when(zh < 2)(lambda: pl.semaphore_wait(ready.at[0], 1))
    pl.when(zh == 0)(lambda: pl.semaphore_wait(ready.at[1], 1))
    for h in range(2):
        cols = pl.ds(HALF * h, HALF)
        swaps[h].wait_recv()
        ph[:, cols] = (br[mine, cols] + bo[mine, cols].astype(F32)).astype(BF)
        near = net.copy(ph.at[:, cols], pr.at[0, mine, cols], "zh", 1, when=zh < 2)
        skip = net.copy(ph.at[:, cols], pr.at[1, mine, cols], "zh", 2, when=zh == 0)
        far.append((near, skip))

    def up2(t, got):
        d = 4 - t
        total = x2sum(d)
        if t > 1:
            got.wait_recv()
            total = total + y2p[t - 2].astype(F32)
        y2s[t - 1] = total.astype(BF)
        return net.copy(y2s.at[t - 1], y2p.at[t - 1], "y", 1)

    def down2(t, got):
        d = t - 5
        total = x2sum(d)
        if t > 1:
            got.wait_recv()
            total = total + y2m[t - 2].astype(F32)
        y2s[2 + t] = total.astype(BF)
        return net.copy(y2s.at[2 + t], y2m.at[t - 1], "y", -1)

    u2 = d2 = None
    for t in range(1, 5):
        d2 = down2(t, d2)
        if t <= 3:
            u2 = up2(t, u2)
        if t <= 3:
            u1 = up1(t + 1, u1)
        if t <= 2:
            d1 = down1(t + 1, d1)
        backward(2 * t - 2, 2 * t)
    for c in u1 + d1:
        c.wait_recv()
    y1[...] = (prod[:, y, :, :, lo].astype(F32) + y1p[3].astype(F32) + y1m[2].astype(F32)).astype(BF)
    x1c = [net.copy(y1.at[:, moved("x", dx)], x1r.at[dx - 1], "x", dx) for dx in (1, 2, 3)]

    total = x2sum(0)
    u2.wait_recv()
    d2.wait_recv()
    total = total + y2p[2].astype(F32) + y2m[3].astype(F32)
    y2[...] = total.astype(BF)
    z2c = [net.copy(y2.at[moved("zl", dz)], z2r.at[dz - 1], "zl", dz) for dz in (1, 2, 3)]

    for c in x1c:
        c.wait_recv()
    total = y1[:, x].astype(F32)
    for j in range(3):
        total = total + x1r[j].astype(F32)
    x1[...] = total.astype(BF)
    z1c = [net.copy(x1.at[moved("zl", dz)], z1r.at[dz - 1], "zl", dz) for dz in (1, 2, 3)]

    for cols, last, sums, got in ((hi, y2, z2r, z2c), (lo, x1, z1r, z1c)):
        for c in got:
            c.wait_recv()
        total = last[z].astype(F32)
        for j in range(3):
            total = total + sums[j].astype(F32)
        gp_ref[:, cols] = total * (1.0 / 128.0)

    passed = []
    for h in range(2):
        cols = pl.ds(HALF * h, HALF)
        near, skip = far[h]
        pl.when(zh > 0)(near.wait_recv)
        a = pr.at[0, mine, cols]
        passed.append((net.copy(a, a, "core", 1, when=zh > 0), zh > 0))
        pl.when(zh == 2)(skip.wait_recv)
        a = pr.at[1, mine, cols]
        passed.append((net.copy(a, a, "core", 1, when=zh == 2), zh == 2))
    br[...] = br[...] + res[...].astype(F32)

    @pl.when(core == 1)
    def _():
        br[...] = br[...] + bo[...].astype(F32)

    for c, when in passed:
        pl.when(when)(c.wait_recv)

    @pl.when(zh > 0)
    def _():
        br[...] = br[...] + pr[0].astype(F32)

    @pl.when(zh == 2)
    def _():
        br[...] = br[...] + pr[1].astype(F32)

    ro[...] = br[...].astype(BF)
    net.drain()


def write_out(*refs):
    sem = refs[10]
    copies = [pltpu.make_async_copy(refs[i], refs[5 + i], sem.at[i]) for i in range(5)]
    for c in copies:
        c.start()
    for c in copies:
        c.wait()


def local(queries, key_rows, value_rows, out_proj, scale_ids, residual_in, cotangent):
    anyspace = pl.BlockSpec(memory_space=pl.ANY)
    vmem = pl.BlockSpec(memory_space=pltpu.VMEM)
    act = jax.ShapeDtypeStruct((T, D), BF)
    V = pltpu.VMEM
    scratch = [V((T, D), BF)] * 5 + [
        V((4, 8, 4, 8, D), BF),
        V((T, T), F32),
        V((16, T, T), BF),
    ] + [V((T, D), BF)] * 2 + [
        V((4, 8, 4, 8, D), BF),
        V((4, 4, 4, 8, HALF), BF),
        V((3, 4, 4, 8, HALF), BF),
        V((4, 4, 8, HALF), BF),
        V((3, 4, 8, HALF), BF),
        V((4, 8, HALF), BF),
        V((3, 8, HALF), BF),
        V((3, 4, 8, 8, HALF), BF),
        V((3, 4, 8, HALF), BF),
        V((4, 4, 8, HALF), BF),
        V((7, 4, 8, HALF), BF),
        V((4, 8, HALF), BF),
        V((3, 8, HALF), BF),
        V((T, D), F32),
        V((T, D), BF),
        V((T, D), BF),
        V((ROWS, D), BF),
        V((2, T, D), BF),
        pltpu.SemaphoreType.DMA((6,)),
        pltpu.SemaphoreType.DMA((COPIES,)),
        pltpu.SemaphoreType.DMA((COPIES,)),
        pltpu.SemaphoreType.REGULAR((2,)),
    ]
    held = (V((T, D), BF),) * 4 + (V((8, D), F32),)
    made = pl.pallas_call(
        kernel,
        out_shape=held,
        in_specs=[anyspace] * 4 + [vmem] + [anyspace] * 2,
        out_specs=(vmem,) * 5,
        scratch_shapes=scratch,
        compiler_params=pltpu.CompilerParams(
            collective_id=0, has_side_effects=True, vmem_limit_bytes=56 << 20
        ),
        name="fused",
    )(
        queries.reshape(T, D), key_rows.reshape(T, D), value_rows.reshape(T, D), out_proj.reshape(8, D),
        scale_ids, residual_in.reshape(T, D), cotangent.reshape(T, D),
    )
    ro, gq, gk, gv, gp = pl.pallas_call(
        write_out,
        out_shape=(act, act, act, act, jax.ShapeDtypeStruct((8, D), F32)),
        in_specs=[vmem] * 5,
        out_specs=(anyspace,) * 5,
        scratch_shapes=[pltpu.SemaphoreType.DMA((5,))],
        name="write_out",
    )(*(pltpu.with_memory_space_constraint(a, pltpu.VMEM) for a in made))
    lead = (1, 1, T, D)
    return ro.reshape(lead), gq.reshape(lead), gk.reshape(lead), gv.reshape(lead), gp.reshape(1, 8, D)


def solution(mesh):
    torus = Mesh(mesh.devices.reshape(tuple(SIZE[a] for a in AXES)), AXES)
    act = P(AA, BA, None, None)
    return jax.shard_map(
        local,
        mesh=torus,
        in_specs=(act, act, act, P(AA, BA, None), P(BA, None), P(BA, None, None), P(BA, None, None)),
        out_specs=(act, act, act, act, P(AA, BA, None)),
        check_vma=False,
    )
```
